32 devices in a mesh: brick: 8 (over z, y), mode: 4 (over x, core).
Axes of the slice: x: 2, y: 2, z: 4, core: 2. Of those that a mesh axis runs over, the one named last changes fastest.
Arguments:
- coeffs: float32 [8192, 3072], P('brick', 'mode'), may hold values from -6 to 6
- weights: bfloat16 [2, 384, 32, 1024], P(None, 'brick'), may hold values from -0.1875 to 0.1875
- owners: int32 [2, 384, 1], P(None, 'brick'), may hold values from 0 to 7; in each aligned block of 48 rows (0 to 47, 48 to 95, ..., all dimensions but the last counted through in order) at most 7 rows name the same one
- offsets: int32 [2, 384], P(None, 'brick'), may hold values from 0 to 7
- mode_basis: bfloat16 [2, 3072, 1024], P(None, 'mode'), may hold values from -0.109375 to 0.109375
- measured: float32 [2, 2048, 1024], P(None, ('brick', 'mode')), may hold values from -6 to 6
Outputs:
- coeffs_out: float32 [8192, 3072], P('brick', 'mode')
- residual: float32 [2, 2048, 1024], P(None, ('brick', 'mode'))
The draws below stay inside these ranges and needn't reach their ends.
Inputs may be any that keep to these rules, and one draw needn't show every extreme that they name: `owners`: among the 48 entries of one brick in one view, no owner is named more than 7 times.
All inputs are finite; a program needn't handle non-finite values.
Results may differ from the reference program's by a relative error of at most 0.0098.
Values may be sent and summed in bfloat16 or wider, within the bound.
No kernel may reach another device: no remote copies, remote signals or barrier semaphores. Data moves between devices by JAX's collectives and lax.ppermute only.
A program may use at most 128 MiB of HBM per device.

```python
import math
import jax
import jax.numpy as jnp
import numpy as np
from jax import lax

M = 3072
BINS = 1024
VOX_DEV = 1024
RB = 32
BLK_DEV = 8
SLOTS = 48
VIEWS = 2
ITERS = 2
CAP = 7
RAYS = 2048
VOX = 8192
N_BRICK = 8


def touch_ends(entries, rng, smallest, top_value):
    dims = entries.shape
    place = [jax.random.randint(jax.random.fold_in(rng, axis), (), 0, dims[axis]) for axis in range(len(dims))]
    entries = entries.at[tuple(place)].set(smallest)
    longest = dims.index(max(dims))
    place[longest] = (place[longest] + 1) % dims[longest]
    return entries.at[tuple(place)].set(top_value)


def levels(stream_key, shape, shards, least, top_value):
    gain = 1.0
    for position, parts in shards:
        draws = jax.random.uniform(jax.random.fold_in(jax.random.fold_in(stream_key, 6), position), (parts,), jnp.float32, least / len(shards), top_value / len(shards))
        gain = gain * jnp.repeat(jnp.exp(draws), shape[position] // parts).reshape((-1,) + (1,) * (len(shape) - 1 - position))
    return gain


def shared_out(own_key, own, number, rows, amount, top, bound, lean):
    order = jax.random.permutation(own_key, amount)
    packed, ordinary = shares(amount, rows * top, bound, lean, True), shares(amount, rows * top, bound, lean, False)
    places = jnp.arange(amount)

    def named(tallies, turn):
        used = int((tallies > 0).sum())
        fixed = max(1, used // 4)
        passed = fixed + (places - fixed + turn * (used - fixed)) % max(1, amount - fixed)
        return jnp.zeros((amount,), jnp.int32).at[order[jnp.where(places < fixed, places, passed)]].set(jnp.asarray(tallies, jnp.int32))

    tallies = jnp.where(number % 4 == 0, named(packed, number // 4), named(ordinary, number - number // 4 - 1))
    mixed = jax.random.permutation(jax.random.fold_in(own, 3), amount)
    giver, taker = mixed[0:amount // 2 * 2:2], mixed[1:amount // 2 * 2:2]
    slack = jnp.minimum(tallies[giver] - 1, bound - tallies[taker]) // 2
    slack = jnp.where((giver == order[0]) | (taker == order[0]) | (tallies[taker] == 0), 0, jnp.maximum(slack, 0))
    passed = jax.random.randint(jax.random.fold_in(own, 4), (amount // 2,), 0, 1 << 20) % (slack + 1)
    tallies = tallies.at[giver].add(-passed).at[taker].add(passed)
    members = jnp.searchsorted(jnp.cumsum(tallies), jnp.arange(rows * top), side="right").astype(jnp.int32)
    table = members.reshape(top, rows).T
    table = table[jax.random.permutation(jax.random.fold_in(own, 1), rows)]
    turn = jax.random.randint(jax.random.fold_in(own, 2), (rows, 1), 0, top)
    return jnp.take_along_axis(table, (jnp.arange(top)[None, :] + turn) % top, axis=1)


def shares(amount, total, reach, slope, full):
    weights = [(1 << 20) // math.isqrt(standing ** slope) + 1 for standing in range(1, amount + 1)]
    largest = reach if full else min(reach, max(-(-total // amount), total * weights[0] // sum(weights)))
    least = 1 if total - largest >= amount - 1 else 0
    given, rest = [largest] + [least] * (amount - 1), total - largest - least * (amount - 1)
    while rest > 0:
        movable = [i for i in range(1, amount) if given[i] < largest] or [i for i in range(1, amount) if given[i] < reach]
        pool, remaining = sum([weights[i] for i in movable]), rest
        for i in movable:
            more = min(reach - given[i], max(1, remaining * weights[i] // pool), rest)
            given[i] = given[i] + more
            rest = rest - more
    return np.array(given)


def normal_values(key, extent, scale, limit, pieces=(), kind=jnp.bfloat16):
    entries = scale * jax.random.normal(key, extent, jnp.float32)
    if pieces:
        entries = entries * levels(key, extent, pieces, -0.22, 0.18)
    return jnp.clip(entries, -limit, limit).astype(kind)


def setup_inputs(seed: int = 0) -> dict:
    key_of = jax.random.split(jax.random.key(seed), 7)
    coeffs = normal_values(key_of[0], (VOX, M), 1.0, 6.0, ((0, 8), (1, 4)), jnp.float32)
    weights = normal_values(key_of[1], (VIEWS, N_BRICK * SLOTS, RB, VOX_DEV), VOX_DEV ** -0.5, 0.1875, ((1, 8),))
    owners_keys = jax.random.split(jax.random.fold_in(key_of[2], 1), VIEWS * (N_BRICK * SLOTS) // SLOTS)
    owners_turns = jax.random.permutation(jax.random.fold_in(key_of[2], 3), VIEWS * (N_BRICK * SLOTS) // SLOTS)
    owners = jax.vmap(lambda own, number: shared_out(jax.random.fold_in(key_of[2], 2), own, number, SLOTS, N_BRICK, 1, CAP, 2))(owners_keys, owners_turns).reshape((VIEWS, N_BRICK * SLOTS, 1))
    offsets = touch_ends(jax.random.randint(key_of[3], (VIEWS, N_BRICK * SLOTS), 0, BLK_DEV), jax.random.fold_in(key_of[3], 1), 0, BLK_DEV - 1).astype(jnp.int32)
    mode_basis = normal_values(key_of[4], (VIEWS, M, BINS), M ** -0.5, 0.109375, ((1, 4),))
    measured = normal_values(key_of[5], (VIEWS, RAYS, BINS), 1.0, 6.0, ((1, 32),), jnp.float32)
    return {"coeffs": coeffs, "weights": weights, "owners": owners, "offsets": offsets, "mode_basis": mode_basis, "measured": measured}


LEARN_RATE = 0.2


def brick_forward(pair_args):
    return jnp.dot(pair_args[0], pair_args[1], preferred_element_type=jnp.float32).astype(jnp.bfloat16)


def brick_adjoint(pair_args):
    return lax.dot_general(pair_args[0], pair_args[1], (((0,), (0,)), ((), ())), preferred_element_type=jnp.float32)


def reference(coeffs, weights, owners, offsets, mode_basis, measured):
    vox_total, mode_total = coeffs.shape
    block_ids = (owners[:, :, 0] * BLK_DEV + offsets).astype(jnp.int32)
    residuals = []
    for step_index in range(ITERS):
        low_coeffs = coeffs.astype(jnp.bfloat16).reshape(N_BRICK, VOX_DEV, mode_total)
        update = jnp.zeros((N_BRICK, VOX_DEV, mode_total), jnp.float32)
        residuals = []
        for view_index in range(VIEWS):
            brick_weights = weights[view_index].reshape(N_BRICK, SLOTS * RB, VOX_DEV)
            slot_proj = lax.map(brick_forward, (brick_weights, low_coeffs))
            slot_proj = slot_proj.reshape(N_BRICK * SLOTS, RB, mode_total)
            summed = jnp.zeros((N_BRICK * BLK_DEV, RB, mode_total), jnp.float32)
            summed = summed.at[block_ids[view_index]].add(slot_proj.astype(jnp.float32))
            low_rays = summed.reshape(RAYS, mode_total).astype(jnp.bfloat16)
            intensity = jnp.dot(low_rays, mode_basis[view_index], preferred_element_type=jnp.float32)
            residual = intensity - measured[view_index]
            residuals.append(residual)
            grad_rays = jnp.dot(residual.astype(jnp.bfloat16), mode_basis[view_index].T,
                                preferred_element_type=jnp.float32).astype(jnp.bfloat16)
            grad_blocks = grad_rays.reshape(N_BRICK * BLK_DEV, RB, mode_total)
            picked = grad_blocks[block_ids[view_index]].reshape(N_BRICK, SLOTS * RB, mode_total)
            update = update + lax.map(brick_adjoint, (brick_weights, picked))
        coeffs = coeffs - LEARN_RATE * update.reshape(vox_total, mode_total)
    return coeffs, jnp.stack(residuals)
```

```python
import functools

import jax
import jax.numpy as jnp
from jax import lax
from jax.experimental import pallas as pl
from jax.experimental.pallas import tpu as pltpu
from jax.sharding import PartitionSpec as P

ITERS = 2
LEARN_RATE = 0.2
F32 = jnp.float32
BF16 = jnp.bfloat16


def axis_bits(size):
    bits = [1 << i for i in range(size.bit_length() - 1)]
    assert 1 << len(bits) == size
    return bits


def swap(x, axis, bit):
    size = lax.axis_size(axis)
    return lax.ppermute(x, axis, [(i, i ^ bit) for i in range(size)])


def place_of(relative, bits):
    place = jnp.zeros_like(relative)
    for level, bit in enumerate(bits):
        place = place + jnp.where((relative & bit) != 0, 1 << (len(bits) - 1 - level), 0)
    return place


def peer_of(place, bits):
    return sum(bit for level, bit in enumerate(bits) if place >> (len(bits) - 1 - level) & 1)


def spread_kernel(place_ref, weight_ref, *refs):
    outs, total = refs[:-1], refs[-1]
    slot_count, ray_block = weight_ref.shape[1:3]

    def clear(block, carry):
        total[block] = jnp.zeros(total.shape[1:], F32)
        return carry

    def add(slot, carry):
        place = place_ref[slot]
        total[place] = total[place] + weight_ref[0, slot].astype(F32)
        return carry

    lax.fori_loop(0, total.shape[0], clear, 0)
    lax.fori_loop(0, slot_count, add, 0)
    first = 0
    for out in outs:
        blocks = out.shape[0] // ray_block

        def store(block, carry, out=out, first=first):
            rows = pl.ds(pl.multiple_of(block * ray_block, ray_block), ray_block)
            out[rows, :] = total[first + block].astype(BF16)
            return carry

        lax.fori_loop(0, blocks, store, 0)
        first += blocks


def spread_weights(weights, view, places, piece_rows):
    _, slot_count, ray_block, voxels = weights.shape
    width = min(256, voxels)
    grid_spec = pltpu.PrefetchScalarGridSpec(
        num_scalar_prefetch=1,
        grid=(voxels // width,),
        in_specs=[pl.BlockSpec((1, slot_count, ray_block, width), lambda j, _: (view, 0, 0, j))],
        out_specs=[pl.BlockSpec((rows, width), lambda j, _: (0, j)) for rows in piece_rows],
        scratch_shapes=[pltpu.VMEM((sum(piece_rows) // ray_block, ray_block, width), F32)],
    )
    return pl.pallas_call(
        spread_kernel,
        grid_spec=grid_spec,
        out_shape=[jax.ShapeDtypeStruct((rows, voxels), BF16) for rows in piece_rows],
        cost_estimate=pl.CostEstimate(
            flops=8 * sum(piece_rows) * voxels,
            bytes_accessed=2 * voxels * (slot_count * ray_block + sum(piece_rows)),
            transcendentals=0,
        ),
        name="spread",
    )(places, weights)


def dot(a, b):
    return jnp.dot(a, b, preferred_element_type=F32)


def dot_t(a, b):
    return lax.dot_general(a, b, (((0,), (0,)), ((), ())), preferred_element_type=F32)


def dot_nt(a, b):
    return lax.dot_general(a, b, (((1,), (1,)), ((), ())), preferred_element_type=F32)


def scatter_sum(products, axis, bits, along):
    arrived = []
    for level, bit in enumerate(bits):
        arrived.append(swap(finish(products[level](), arrived, along).astype(BF16), axis, bit))
        arrived = trim(arrived, products, level, along)
    return finish(products[len(bits)](), arrived, along)


def finish(term, arrived, along):
    size = term.shape[along]
    for other in arrived:
        part = lax.slice_in_dim(other, other.shape[along] - size, None, axis=along)
        term = term + part.astype(F32)
    return term


def trim(arrived, products, level, along):
    kept = []
    for index, other in enumerate(arrived):
        if index == len(arrived) - 1:
            kept.append(other)
        else:
            kept.append(lax.slice_in_dim(other, 0, other.shape[along] // 2, axis=along))
    return kept


def collect(piece, axis, bits):
    held = piece
    arrived = []
    for bit in reversed(bits):
        other = swap(held, axis, bit)
        arrived.append(other)
        held = jnp.concatenate([held, other], axis=0)
    return arrived


def shards(coeffs, weights, owners, offsets, mode_basis, measured):
    bricks, parts = lax.axis_size("brick"), lax.axis_size("mode")
    brick_bits, mode_bits = axis_bits(bricks), axis_bits(parts)
    views, slot_count, ray_block, voxels = weights.shape
    rows_here, bins = measured.shape[1:]
    rows = rows_here * parts
    width = bins // parts
    blocks = rows // ray_block
    here, part = lax.axis_index("brick"), lax.axis_index("mode")

    relative = owners[:, :, 0] ^ here
    places = place_of(relative, brick_bits) * blocks + offsets
    piece_rows = [rows] + [rows << i for i in range(len(brick_bits))]

    basis = []
    for view in range(views):
        cols = [
            lax.dynamic_slice(
                mode_basis[view], (0, (part ^ peer_of(place, mode_bits)) * width), (mode_basis.shape[1], width)
            )
            for place in range(parts)
        ]
        pieces = [cols[0]]
        for level in range(len(mode_bits)):
            count = 1 << level
            pieces.append(jnp.concatenate(cols[count : 2 * count], axis=1))
        basis.append(pieces)

    spread = [spread_weights(weights, view, places[view], piece_rows) for view in range(views)]

    turned = measured.reshape(views, rows_here, parts, width).transpose(2, 0, 1, 3)
    turned = lax.all_to_all(turned, "mode", 0, 0, tiled=True)
    wanted = turned.transpose(1, 0, 2, 3).reshape(views, rows, width)

    residuals = []
    for step_index in range(ITERS):
        low = coeffs.astype(BF16)
        residuals = []
        update = None
        for view in range(views):
            products = [
                functools.partial(dot, low, piece) for piece in reversed(basis[view])
            ]
            pattern = scatter_sum(products, "mode", mode_bits, 1).astype(BF16)
            products = [
                functools.partial(dot, piece, pattern) for piece in reversed(spread[view])
            ]
            residual = scatter_sum(products, "brick", brick_bits, 0) - wanted[view]
            residuals.append(residual)
            rays = residual.astype(BF16)
            back = dot_t(spread[view][0], rays)
            for piece, other in zip(spread[view][1:], collect(rays, "brick", brick_bits)):
                back = back + dot_t(piece, other)
            back = back.astype(BF16)
            term = dot_nt(back, basis[view][0])
            held = back
            for level, bit in enumerate(reversed(mode_bits)):
                other = swap(held, "mode", bit)
                term = term + dot_nt(other, basis[view][level + 1])
                held = jnp.concatenate([held, other], axis=1)
            update = term if update is None else update + term
        coeffs = coeffs - LEARN_RATE * update
    residual = jnp.stack(residuals).reshape(views, parts, rows_here, width).transpose(1, 0, 2, 3)
    residual = lax.all_to_all(residual, "mode", 0, 0, tiled=True)
    residual = residual.transpose(1, 2, 0, 3).reshape(views, rows_here, bins)
    return (coeffs, residual)


def solution(mesh):
    return jax.shard_map(
        shards,
        mesh=mesh,
        in_specs=(
            P("brick", "mode"),
            P(None, "brick", None, None),
            P(None, "brick", None),
            P(None, "brick"),
            P(None, "mode", None),
            P(None, ("brick", "mode"), None),
        ),
        out_specs=(P("brick", "mode"), P(None, ("brick", "mode"), None)),
        check_vma=False,
    )
```
